64 devices in a mesh: dp: 4 (over x, y), pp: 16 (over z, core).
Axes of the slice: x: 2, y: 2, z: 8, core: 2. Of those that a mesh axis runs over, the one named last changes fastest.
The devices are a block of a 4x4x8 slice.
Arguments:
- x_final: bfloat16 [8192, 768], P(('dp', 'pp')), parts along dimension 0
- w_vocab: bfloat16 [50304, 768], P('pp')
- labels: int32 [8192], P('dp'), parts along dimension 0
- tok_mask: int32 [8192], P('dp'), parts along dimension 0
- next_ids: int32 [8192], P('dp'), parts along dimension 0
- d_embed: bfloat16 [8192, 768], P(('dp', 'pp')), parts along dimension 0
- act_in: bfloat16 [64, 2048, 768], P(('dp', 'pp')), parts along dimension 0
- w_up: bfloat16 [16, 768, 3072], P('pp')
- w_down: bfloat16 [16, 3072, 768], P('pp')
Outputs:
- output 1: float32 [4], P('dp'), parts along dimension 0
- output 2: float32 [8192, 768], P(('dp', 'pp')), parts along dimension 0
- output 3: bfloat16 [201216, 768], P(('dp', 'pp')), parts along dimension 0
- output 4: bfloat16 [8192, 768], P(('dp', 'pp')), parts along dimension 0
- output 5: bfloat16 [64, 2048, 768], P(('dp', 'pp')), parts along dimension 0
There are 4 independent parts. The reference program is written for one: setup_inputs(seed, part) draws one part's arguments, and reference() takes and returns one part's arrays. A program takes and returns all parts, laid end to end along the dimension named above; an argument that names none is the same for every part.
All inputs are finite; a program needn't handle non-finite values.
Results may differ from the reference program's by a relative error of at most 0.001.
Values are sent between devices in bfloat16 or wider.
A program may use at most 768 MiB of HBM per device.

```python
import jax
import jax.numpy as jnp
from jax import lax

MODEL_DIM = 768
VOCAB_SIZE = 50304
HIDDEN_DIM = 3072
STAGES = 16
TOKENS = 2048


def setup_inputs(seed: int = 0, part: int = 0) -> dict:
    base = jax.random.key(seed)
    shared = jax.random.split(base, 3)
    part_key = jax.random.fold_in(base, part)
    own = jax.random.split(part_key, 7)
    logit_scale = 2.5 * MODEL_DIM ** -0.5
    w_vocab = (jax.random.normal(shared[0], (VOCAB_SIZE, MODEL_DIM), jnp.float32) * logit_scale).astype(jnp.bfloat16)
    w_up = (jax.random.normal(shared[1], (STAGES, MODEL_DIM, HIDDEN_DIM), jnp.float32) * MODEL_DIM ** -0.5).astype(jnp.bfloat16)
    w_down = (jax.random.normal(shared[2], (STAGES, HIDDEN_DIM, MODEL_DIM), jnp.float32) * HIDDEN_DIM ** -0.5).astype(jnp.bfloat16)
    x_final = jax.random.normal(own[0], (TOKENS, MODEL_DIM), jnp.float32).astype(jnp.bfloat16)
    labels = jax.random.randint(own[1], (TOKENS,), 0, VOCAB_SIZE, jnp.int32).at[0].set(VOCAB_SIZE - 1).at[1].set(0)
    tok_mask = (jax.random.randint(own[2], (TOKENS,), 0, 20, jnp.int32) != 0).astype(jnp.int32)
    next_ids = jax.random.randint(own[3], (TOKENS,), 0, VOCAB_SIZE, jnp.int32).at[0].set(0).at[1].set(VOCAB_SIZE - 1)
    d_embed = (jax.random.normal(own[4], (TOKENS, MODEL_DIM), jnp.float32) / (TOKENS * MODEL_DIM ** 0.5)).astype(jnp.bfloat16)
    act_in = jax.random.normal(own[5], (STAGES, TOKENS, MODEL_DIM), jnp.float32).astype(jnp.bfloat16)
    return dict(x_final=x_final, w_vocab=w_vocab, labels=labels, tok_mask=tok_mask, next_ids=next_ids, d_embed=d_embed, act_in=act_in, w_up=w_up, w_down=w_down)


def mlp_layer(blocks):
    act_rows, w_first, w_second = blocks
    hidden = jax.nn.gelu(jnp.dot(act_rows, w_first, preferred_element_type=jnp.float32)).astype(jnp.bfloat16)
    return (act_rows.astype(jnp.float32) + jnp.dot(hidden, w_second, preferred_element_type=jnp.float32)).astype(jnp.bfloat16)


def reference(x_final, w_vocab, labels, tok_mask, next_ids, d_embed, act_in, w_up, w_down):
    emb_scale = MODEL_DIM ** 0.5
    logits = jnp.dot(x_final, w_vocab.T, preferred_element_type=jnp.float32)
    log_total = jax.nn.logsumexp(logits, axis=1)
    token_rows = jnp.arange(TOKENS)
    target = logits[token_rows, labels]
    weight = tok_mask.astype(jnp.float32)
    kept_count = jnp.maximum(jnp.sum(weight), 1.0)
    mean_loss = jnp.sum(weight * (log_total - target)) / kept_count
    probs = jnp.exp(logits - log_total[:, None])
    grad_logits = (probs.at[token_rows, labels].add(-1.0) * (weight / kept_count)[:, None]).astype(jnp.bfloat16)
    d_hidden = jnp.dot(grad_logits, w_vocab, preferred_element_type=jnp.float32)
    d_head = jnp.dot(grad_logits.T, x_final, preferred_element_type=jnp.float32)
    d_table = jax.ops.segment_sum(d_embed.astype(jnp.float32), next_ids, num_segments=VOCAB_SIZE)
    d_vocab = (d_head + d_table * emb_scale).astype(jnp.bfloat16)
    embed_out = (w_vocab[next_ids].astype(jnp.float32) * emb_scale).astype(jnp.bfloat16)
    mlp_out = lax.map(mlp_layer, (act_in, w_up, w_down))
    return mean_loss.reshape(1), d_hidden, d_vocab, embed_out, mlp_out
```

```python
import functools
import math

import jax
import jax.numpy as jnp
from jax import lax
from jax.experimental import pallas as pl
from jax.experimental.pallas import tpu as pltpu
from jax.sharding import PartitionSpec as P

MESH = pl.DeviceIdType.MESH
F32 = jnp.float32
BF16 = jnp.bfloat16
QT = 640
WT = 160
NEG = -1e30


def body(
    n, vocab, emb_scale,
    x_in, d_in, w_hbm, lab_ref, ids_ref, mask_ref, act_hbm, w1_hbm, w2_hbm, emb_hbm,
    dx_out, dw_hbm, h0_out, y_hbm, loss_out,
    wv, wt, xg, dg, dxo, dxp, dxr, ho, hp, hr, stat_rx, tp_rx, stat_tx, tp_tx, mst, scale, wgt,
    x_ss, x_rs, x_ps, x_pr, d_ss, d_rs, d_ps, d_pr,
    r_ss, r_rs, r_ps, r_pr, h_ss, h_rs, h_ps, h_pr, st_ss, st_rs, tp_ss, tp_rs, loc, e_sem,
):
    ring = n // 2
    hb, dim = x_in.shape
    half = hb // 2
    tb = 2 * hb
    dhalf = dim // 2
    vpad = wv.shape[0]
    nq = vpad // QT
    nw = vpad // WT
    me = lax.axis_index("pp")
    j = me // 2
    c = lax.rem(me, 2)
    oc = 1 - c
    chip = lambda k: lax.rem(j + k + 2 * ring, ring)
    core = lambda k: {"pp": 2 * chip(k) + c}
    partner = {"pp": 2 * j + oc}
    FAR = (0, 1)
    SIGN = (1, -1)

    wv[vpad - 64:, :] = jnp.zeros((64, dim), BF16)
    w_load = pltpu.make_async_copy(w_hbm, wv.at[pl.ds(0, vocab)], loc.at[0])
    w_load.start()

    barrier = pltpu.get_barrier_semaphore()
    for p in range(1, n):
        pl.semaphore_signal(barrier, inc=1, device_id={"pp": lax.rem(me + p, n)}, device_id_type=MESH)
    pl.semaphore_wait(barrier, n - 1)

    def remote(src, dst, ss, rs, dev):
        return pltpu.make_async_remote_copy(src_ref=src, dst_ref=dst, send_sem=ss, recv_sem=rs, device_id=dev, device_id_type=MESH)

    def gather_flow(src, buf, ss, rs, ps, pr):
        def rows(origin, cc, h):
            return buf.at[pl.ds(pl.multiple_of(origin * tb + cc * hb + h * half, half), half)]

        def send(d, s, h):
            origin = chip(-SIGN[d] * s)
            ref = src.at[pl.ds(h * half, half)] if s == 0 else rows(origin, c, h)
            return remote(ref, rows(origin, c, h), ss.at[d, s, h], rs.at[d, s, h], core(SIGN[d]))

        def share(d, s, h):
            origin = chip(-SIGN[d] * (s + 1))
            return remote(rows(origin, c, h), rows(origin, c, h), ps.at[d, s, h], pr.at[d, s, h], partner)

        def share_in(d, s, h):
            origin = chip(-SIGN[d] * (s + 1))
            return remote(rows(origin, oc, h), rows(origin, oc, h), ps.at[d, s, h], pr.at[d, s, h], partner)

        def own():
            mine = buf.at[pl.ds(pl.multiple_of(j * tb + c * hb, hb), hb)]
            return remote(src, mine, ps.at[0, 3, 1], pr.at[0, 3, 1], partner)

        def start():
            for k in range(2):
                for d in range(2):
                    send(d, 0, FAR[d] if k == 0 else 1 - FAR[d]).start()
            own().start()
            buf[pl.ds(pl.multiple_of(j * tb + c * hb, hb), hb), :] = src[...]

        units = [(s, k) for s in range(4) for k in range(2) if s < 3 or k == 0]

        def event(e):
            s, k = units[e]
            for d in range(2):
                h = FAR[d] if k == 0 else 1 - FAR[d]
                send(d, s, h).wait_recv()
                if s < 2 or (s == 2 and k == 0):
                    send(d, s + 1, h).start()
                share(d, s, h).start()

        def finish():
            for s, k in units:
                for d in range(2):
                    h = FAR[d] if k == 0 else 1 - FAR[d]
                    share_in(d, s, h).wait_recv()
            own().wait_recv()

        def drain():
            for s, k in units:
                for d in range(2):
                    h = FAR[d] if k == 0 else 1 - FAR[d]
                    send(d, s, h).wait_send()
                    share(d, s, h).wait_send()
            own().wait_send()

        return start, event, finish, drain, len(units)

    def scatter_flow(away, own, pbuf, rx, ss, rs, ps, pr, length):
        def share(b, k):
            return remote(away(b, oc), pbuf.at[b], ps.at[k], pr.at[k], partner)

        def part(ref, h):
            return ref.at[pl.ds(h * length, length)]

        def send(d, k, h):
            return remote(part(rx.at[d, k], h), part(rx.at[d, k - 1], h), ss.at[d, k, h], rs.at[d, k - 1, h], core(SIGN[d]))

        def emit(d, k, far, first):
            h = FAR[d] if far else 1 - FAR[d]
            b = chip(SIGN[d] * k)
            if first:
                part(rx.at[d, k], h)[...] = part(own(b), h)[...] + part(pbuf.at[b], h)[...]
            else:
                send(d, k + 1, h).wait_recv()
                part(rx.at[d, k], h)[...] = part(rx.at[d, k], h)[...] + (part(own(b), h)[...] + part(pbuf.at[b], h)[...])
            send(d, k, h).start()

        def final(out):
            for far in (False, True):
                for d in range(2):
                    send(d, 1, FAR[d] if far else 1 - FAR[d]).wait_recv()
            out[...] = (own(j)[...] + pbuf[j]) + (rx[0, 0] + rx[1, 0])

        def drain():
            for d in range(2):
                for k, far in ((4, True), (3, False), (3, True), (2, False), (2, True), (1, False), (1, True)):
                    send(d, k, FAR[d] if far else 1 - FAR[d]).wait_send()

        return share, emit, final, drain

    x_start, x_event, x_finish, x_drain, n_units = gather_flow(x_in, xg, x_ss, x_rs, x_ps, x_pr)
    d_start, d_event, d_finish, d_drain, _ = gather_flow(d_in, dg, d_ss, d_rs, d_ps, d_pr)
    h_share, h_emit, h_final, h_drain = scatter_flow(
        lambda b, cc: emb_hbm.at[pl.ds(pl.multiple_of(b * tb + cc * hb, hb), hb)], lambda b: ho.at[b], hp, hr, h_ss, h_rs, h_ps, h_pr, half)
    r_share, r_emit, r_final, r_drain = scatter_flow(
        lambda b, cc: dxo.at[b, cc], lambda b: dxo.at[b, c], dxp, dxr, r_ss, r_rs, r_ps, r_pr, dhalf)

    x_start()
    for k in range(ring):
        h_share(lax.rem(j + k, ring), k).start()

    def e_load(b):
        return pltpu.make_async_copy(emb_hbm.at[pl.ds(pl.multiple_of(b * tb + c * hb, hb), hb)], ho.at[b], e_sem.at[b])

    for b in range(ring):
        e_load(b).start()

    def h_partner_wait():
        for k in range(ring):
            h_share(lax.rem(j + k, ring), k).wait_recv()
            e_load(k).wait()

    def h_both(k, far, first):
        for d in range(2):
            h_emit(d, k, far, first)

    def h_init():
        h_partner_wait()
        h_both(4, True, True)
        h_both(3, False, True)

    side = [
        h_init, d_start,
        lambda: h_both(3, True, False), lambda: d_event(0),
        lambda: h_both(2, False, False), lambda: d_event(1),
        lambda: h_both(2, True, False), lambda: d_event(2),
        lambda: h_both(1, False, False), lambda: d_event(3),
        lambda: h_both(1, True, False), lambda: d_event(4),
        lambda: d_event(5), lambda: d_event(6),
    ]

    def at(index, table):
        for when, todo in table:
            pl.when(index == when)(todo)

    chunk = tb
    n_chunks = act_hbm.shape[0] // chunk
    hid = w1_hbm.shape[1]

    w_load.wait()

    @pl.loop(0, vpad // 128)
    def _(t):
        o = pl.multiple_of(t * 128, 128)
        wt[:, pl.ds(o, 128)] = wv[pl.ds(o, 128), :].T

    def mlp(w1v, w2v, abuf, ybuf, hbuf, wsem, asem, ysem):
        c1 = pltpu.make_async_copy(w1_hbm, w1v, wsem.at[0])
        c2 = pltpu.make_async_copy(w2_hbm, w2v, wsem.at[1])
        c1.start()
        c2.start()

        def a_copy(i):
            slot = lax.rem(i, 2)
            return pltpu.make_async_copy(act_hbm.at[pl.ds(pl.multiple_of(i * chunk, chunk), chunk)], abuf.at[slot], asem.at[slot])

        def y_copy(i):
            slot = lax.rem(i, 2)
            return pltpu.make_async_copy(ybuf.at[slot], y_hbm.at[pl.ds(pl.multiple_of(i * chunk, chunk), chunk)], ysem.at[slot])

        a_copy(0).start()
        c1.wait()
        c2.wait()
        first = [(2, lambda: x_event(1)), (3, lambda: x_event(2)), (4, lambda: x_event(4)), (5, lambda: x_event(5)), (6, side[0]), (7, side[1])]
        second = [(1, lambda: x_event(0)), (3, lambda: x_event(3)), (5, lambda: x_event(6)), (7, side[2])]

        @pl.loop(0, n_chunks)
        def _(i):
            slot = lax.rem(i, 2)
            a_copy(i).wait()

            @pl.when(i + 1 < n_chunks)
            def _():
                a_copy(i + 1).start()

            a = abuf[slot]
            step = min(512, hid)
            for t in range(hid // step):
                up = jnp.dot(a, w1v[:, t * step:(t + 1) * step], preferred_element_type=F32)
                hbuf[:, t * step:(t + 1) * step] = jax.nn.gelu(up).astype(BF16)
            at(i, first)

            @pl.when(i >= 2)
            def _():
                y_copy(i - 2).wait()

            ybuf[slot] = (abuf[slot].astype(F32) + jnp.dot(hbuf[...], w2v[...], preferred_element_type=F32)).astype(BF16)
            y_copy(i).start()
            at(i, second)

        y_copy(n_chunks - 2).wait()
        y_copy(n_chunks - 1).wait()

    pl.run_scoped(
        mlp,
        pltpu.VMEM(w1_hbm.shape, BF16), pltpu.VMEM(w2_hbm.shape, BF16),
        pltpu.VMEM((2, chunk, dim), BF16), pltpu.VMEM((2, chunk, dim), BF16), pltpu.VMEM((chunk, hid), BF16),
        pltpu.SemaphoreType.DMA((2,)), pltpu.SemaphoreType.DMA((2,)), pltpu.SemaphoreType.DMA((2,)),
    )

    def head(z):
        x_finish()
        kept = mask_ref[...]
        count = jnp.maximum(jnp.sum(kept, keepdims=True), 1.0)
        wgt[...] = kept / count

        def row_iota(rows):
            return lax.broadcasted_iota(jnp.int32, (rows, tb), 0)

        @pl.loop(0, ring)
        def _(b):
            xb = xg[pl.ds(pl.multiple_of(b * tb, tb), tb), :]
            lab = lab_ref[pl.ds(b, 1), :]
            tops, sums, tgt = [], [], jnp.zeros((1, tb), F32)
            def logits(q):
                zt = lax.dot_general(wv[q * QT:(q + 1) * QT, :], xb, (((1,), (1,)), ((), ())), preferred_element_type=F32)
                if (q + 1) * QT > vocab:
                    zt = jnp.where(row_iota(QT) + q * QT < vocab, zt, NEG)
                z[b, q * QT:(q + 1) * QT, :] = zt

            logits(0)
            for q in range(nq):
                if q + 1 < nq:
                    logits(q + 1)
                part = z.at[b, pl.ds(q * QT, QT)]
                top = jnp.max(part[...], axis=0, keepdims=True)
                zt = part[...]
                e = jnp.exp(zt - top)
                part[...] = e
                tgt = tgt + jnp.sum(jnp.where(row_iota(QT) + q * QT == lab, zt, 0.0), axis=0, keepdims=True)
                sums.append(jnp.sum(e, axis=0, keepdims=True))
                tops.append(top)
                mst[q, pl.ds(b, 1), :] = top
            peak = functools.reduce(jnp.maximum, tops)
            total = sum(s * jnp.exp(t - peak) for s, t in zip(sums, tops))
            stat_tx[pl.ds(b, 1), :] = peak + jnp.log(total)
            tp_tx[pl.ds(b, 1), :] = tgt * mask_ref[pl.ds(b, 1), :]
            at(b, [(k, side[3 + k]) for k in range(8)])

        def stat_copy(p):
            return remote(stat_tx, stat_rx.at[me], st_ss.at[p], st_rs.at[p], {"pp": lax.rem(me + p, n)})

        def tp_copy(p):
            return remote(tp_rx.at[pl.ds(n, 1)], tp_rx.at[pl.ds(me, 1)], tp_ss.at[p], tp_rs.at[p], {"pp": lax.rem(me + p, n)})

        order = [n // 2] + [q for k in range(1, n // 2) for q in (n // 2 - k, n // 2 + k)]
        for p in order:
            stat_copy(p).start()
        stat_rx[me] = stat_tx[...]
        mine = jnp.sum(tp_tx[...], keepdims=True)
        tp_rx[pl.ds(n, 1), :] = jnp.broadcast_to(mine, (1, 128))
        tp_rx[pl.ds(me, 1), :] = jnp.broadcast_to(mine, (1, 128))
        for p in order:
            tp_copy(p).start()
        for p in range(1, n):
            stat_copy(p).wait_recv()
        peak = stat_rx[0]
        for p in range(1, n):
            peak = jnp.maximum(peak, stat_rx[p])
        total = jnp.exp(stat_rx[0] - peak)
        for p in range(1, n):
            total = total + jnp.exp(stat_rx[p] - peak)
        lse = peak + jnp.log(total)
        for q in range(nq):
            scale[q] = jnp.exp(mst[q] - lse) * wgt[...]
        lse_sum = jnp.sum(kept * lse, keepdims=True)

        def r_both(k, far, first):
            for d in range(2):
                r_emit(d, k, far, first)

        def dest(t):
            k = jnp.where(t == 0, 4, 3 - (t - 1) // 2)
            k = jnp.where(t == 0, 4, k * (1 - 2 * lax.rem(jnp.maximum(t - 1, 0), 2)))
            return chip(k)

        def pw(t):
            r_share(dest(t), t).wait_recv()

        def first_4():
            pw(0)
            r_both(4, True, True)

        def first_3r():
            pw(1)
            r_emit(0, 3, False, True)

        def first_3l():
            pw(2)
            r_emit(1, 3, False, True)

        def acc_2():
            pw(3)
            pw(4)
            r_both(2, False, False)

        dx_events = [
            (1, first_4), (2, first_3r), (3, first_3l), (4, lambda: r_both(3, True, False)),
            (6, acc_2), (7, lambda: r_both(2, True, False)),
        ]
        dx_side = [(0, side[11]), (1, side[12]), (3, side[13]), (5, lambda: h_final(h0_out))]

        def blocks(gbuf):
            @pl.loop(0, ring)
            def _(t):
                b = dest(t)
                lab = lab_ref[pl.ds(b, 1), :]
                wrow = wgt[pl.ds(b, 1), :]
                for q in range(nq):
                    g = z[b, q * QT:(q + 1) * QT, :] * scale[q, pl.ds(b, 1), :]
                    g = g - jnp.where(row_iota(QT) + q * QT == lab, wrow, 0.0)
                    gbuf[q * QT:(q + 1) * QT, :] = g.astype(BF16)
                @pl.loop(0, dim // 256)
                def _(m):
                    o = pl.multiple_of(m * 256, 256)
                    res = jnp.dot(wt[pl.ds(o, 256), :], gbuf[...], preferred_element_type=F32)
                    dxo[b, 0, pl.ds(o, 256), :] = res[:, :hb]
                    dxo[b, 1, pl.ds(o, 256), :] = res[:, hb:]

                r_share(b, t).start()
                at(t, dx_events)
                at(t, dx_side)

        pl.run_scoped(blocks, pltpu.VMEM((vpad, tb), BF16))
        def tables(gt, ht, wbuf, wsem):
            def w_copy(i, rows):
                slot = lax.rem(i, 2)
                return pltpu.make_async_copy(wbuf.at[slot, pl.ds(0, rows)], dw_hbm.at[pl.ds(pl.multiple_of(i * WT, 8), rows)], wsem.at[slot])

            tail = vocab - (nw - 1) * WT

            def acc_1():
                pw(5)
                pw(6)
                r_both(1, False, False)

            dw_events = [(2, acc_1), (7, lambda: r_both(1, True, False))]

            @pl.loop(0, nw)
            def _(i):
                o = pl.multiple_of(i * WT, WT)
                q = i // (QT // WT)
                slot = lax.rem(i, 2)
                rid = row_iota(WT) + i * WT
                for b in range(ring):
                    g = z[b, pl.ds(o, WT), :] * scale[q, b:b + 1, :]
                    g = g - jnp.where(rid == lab_ref[b:b + 1, :], wgt[b:b + 1, :], 0.0)
                    gt[:, b * tb:(b + 1) * tb] = g.astype(BF16)
                    ht[:, b * tb:(b + 1) * tb] = jnp.where(rid == ids_ref[b:b + 1, :], 1.0, 0.0).astype(BF16)
                @pl.when(i >= 2)
                def _():
                    w_copy(i - 2, WT).wait()

                for t in range(dim // 256):
                    cols = slice(t * 256, (t + 1) * 256)
                    head_part = jnp.dot(gt[...], xg[:, cols], preferred_element_type=F32)
                    table_part = jnp.dot(ht[...], dg[:, cols], preferred_element_type=F32)
                    wbuf[slot, :, cols] = (head_part + table_part * emb_scale).astype(BF16)

                @pl.when(i < nw - 1)
                def _():
                    w_copy(i, WT).start()

                at(i, dw_events)

            w_copy(nw - 1, tail).start()
            w_copy(nw - 2, WT).wait()
            w_copy(nw - 1, tail).wait()

        d_finish()
        pl.run_scoped(
            tables,
            pltpu.VMEM((WT, ring * tb), BF16), pltpu.VMEM((WT, ring * tb), BF16),
            pltpu.VMEM((2, WT, dim), BF16), pltpu.SemaphoreType.DMA((2,)),
        )
        pw(7)
        r_final(dx_out)
        for p in range(1, n):
            tp_copy(p).wait_recv()
        target = jnp.sum(tp_rx[0:n, :], axis=0, keepdims=True)
        loss_out[...] = jnp.broadcast_to((lse_sum - target) / count, loss_out.shape)
        for p in range(1, n):
            stat_copy(p).wait_send()
            tp_copy(p).wait_send()
        for t in range(ring):
            r_share(dest(jnp.int32(t)), t).wait_send()

    pl.run_scoped(
        head,
        pltpu.VMEM((ring, vpad, tb), F32),
    )
    x_drain()
    d_drain()
    r_drain()
    h_drain()
    for k in range(ring):
        h_share(lax.rem(j + k, ring), k).wait_send()


def solution(mesh):
    n = mesh.shape["pp"]
    ring = n // 2

    def local_step(x_rows, w_slice, labels, tok_mask, next_ids, d_rows, act_in, w_up, w_down):
        vocab, dim = w_slice.shape
        hb = x_rows.shape[0]
        tb = 2 * hb
        vpad = -(-vocab // QT) * QT
        emb_scale = math.sqrt(dim)
        offset = lax.axis_index("pp") * vocab
        lab = labels - offset
        lab = jnp.where((lab >= 0) & (lab < vocab), lab, -1).reshape(ring, tb)
        pos = next_ids - offset
        mask = tok_mask.astype(F32).reshape(ring, tb)
        in_share = (pos >= 0) & (pos < vocab)
        picked = w_slice[jnp.clip(pos, 0, vocab - 1)]
        emb = jnp.where(in_share[:, None], picked.astype(F32) * emb_scale, 0.0).astype(BF16)
        vmem = pl.BlockSpec(memory_space=pltpu.VMEM)
        hbm = pl.BlockSpec(memory_space=pltpu.HBM)
        dma = lambda *s: pltpu.SemaphoreType.DMA(s)
        dx, dw, h0, y, loss = pl.pallas_call(
            functools.partial(body, n, vocab, emb_scale),
            out_shape=[
                jax.ShapeDtypeStruct((dim, hb), F32),
                jax.ShapeDtypeStruct((vocab, dim), BF16),
                jax.ShapeDtypeStruct((hb, dim), BF16),
                jax.ShapeDtypeStruct(act_in.shape[1:], BF16),
                jax.ShapeDtypeStruct((8, 128), F32),
            ],
            in_specs=[vmem, vmem, hbm, vmem, vmem, vmem, hbm, hbm, hbm, hbm],
            out_specs=[vmem, hbm, vmem, hbm, vmem],
            scratch_shapes=[
                pltpu.VMEM((vpad, dim), BF16), pltpu.VMEM((dim, vpad), BF16),
                pltpu.VMEM((ring * tb, dim), BF16), pltpu.VMEM((ring * tb, dim), BF16),
                pltpu.VMEM((ring, 2, dim, hb), F32), pltpu.VMEM((ring, dim, hb), F32), pltpu.VMEM((2, 5, dim, hb), F32),
                pltpu.VMEM((ring, hb, dim), BF16), pltpu.VMEM((ring, hb, dim), BF16), pltpu.VMEM((2, 5, hb, dim), BF16),
                pltpu.VMEM((n, ring, tb), F32), pltpu.VMEM((n + 8, 128), F32),
                pltpu.VMEM((ring, tb), F32), pltpu.VMEM((ring, tb), F32),
                pltpu.VMEM((vpad // QT, ring, tb), F32), pltpu.VMEM((vpad // QT, ring, tb), F32), pltpu.VMEM((ring, tb), F32),
            ] + [dma(2, 4, 2)] * 8 + [dma(2, 5, 2), dma(2, 5, 2), dma(ring), dma(ring)] * 2 + [dma(n)] * 4 + [dma(1), dma(ring)],
            compiler_params=pltpu.CompilerParams(collective_id=0, has_side_effects=True, vmem_limit_bytes=67043328),
        )(x_rows, d_rows, w_slice, lab, jnp.where(in_share, pos, -1).reshape(ring, tb), mask, act_in[0], w_up[0], w_down[0], emb)
        return loss[0, :1], dx.T, dw, h0, y[None]

    token_spec = P(("dp", "pp"))
    return jax.shard_map(
        local_step,
        mesh=mesh,
        in_specs=(token_spec, P("pp"), P("dp"), P("dp"), P("dp"), token_spec, token_spec, P("pp"), P("pp")),
        out_specs=(P("dp"), token_spec, token_spec, token_spec, token_spec),
        check_vma=False,
    )
```

```python
import functools
import math

import jax
import jax.numpy as jnp
from jax import lax
from jax.experimental import pallas as pl
from jax.experimental.pallas import tpu as pltpu
from jax.sharding import PartitionSpec as P

MESH = pl.DeviceIdType.MESH
F32 = jnp.float32
BF16 = jnp.bfloat16
QT = 320
WT = 320
NEG = -1e30
OUTER, INNER = True, False
FIRST, LATER = True, False
NT = (((1,), (1,)), ((), ()))
TN = (((0,), (0,)), ((), ()))
ALL = ...
PICK = 256


def down(x):
    return jnp.sum(x, axis=0, keepdims=True)


def body(
    n, vocab,
    x_in, d_in, w_hbm, lab_ref, mask_ref, act_hbm, w1_hbm, w2_hbm, emb_hbm,
    dx_out, dw_hbm, h0_out, y_hbm, loss_out, dg_hbm,
    wv, wt, xg, dxo, dxp, dxr, ho, hp, hr, stat_rx, tp_rx, stat_tx, tp_tx, mst, scale, wgt,
    x_ss, x_rs, x_ps, x_pr, d_ss, d_rs, d_ps, d_pr,
    r_ss, r_rs, r_ps, r_pr, h_ss, h_rs, h_ps, h_pr, st_ss, st_rs, tp_ss, tp_rs, loc, e_sem,
):
    ring = n // 2
    hb, dim = x_in.shape
    half = hb // 2
    tb = 2 * hb
    dhalf = dim // 2
    vpad = wv.shape[0]
    nq = vpad // QT
    nw = vpad // WT
    me = lax.axis_index("pp")
    j = me // 2
    c = lax.rem(me, 2)
    oc = 1 - c
    chip = lambda k: lax.rem(j + k + 2 * ring, ring)
    core = lambda k: {"pp": 2 * chip(k) + c}
    partner = {"pp": 2 * j + oc}
    FAR = (0, 1)
    SIGN = (1, -1)

    wv[vpad - 64:, :] = jnp.zeros((64, dim), BF16)
    w_load = pltpu.make_async_copy(w_hbm, wv.at[pl.ds(0, vocab)], loc.at[0])

    barrier = pltpu.get_barrier_semaphore()
    for p in range(1, n):
        pl.semaphore_signal(barrier, inc=1, device_id={"pp": lax.rem(me + p, n)}, device_id_type=MESH)

    def remote(src, dst, ss, rs, dev):
        return pltpu.make_async_remote_copy(src_ref=src, dst_ref=dst, send_sem=ss, recv_sem=rs, device_id=dev, device_id_type=MESH)

    def gather_flow(src, buf, ss, rs, ps, pr, keep_sem=None):
        def rows(origin, cc, h):
            return buf.at[pl.ds(pl.multiple_of(origin * tb + cc * hb + h * half, half), half)]

        def send(d, s, h):
            origin = chip(-SIGN[d] * s)
            ref = src.at[pl.ds(h * half, half)] if s == 0 else rows(origin, c, h)
            return remote(ref, rows(origin, c, h), ss.at[d, s, h], rs.at[d, s, h], core(SIGN[d]))

        def share(d, s, h):
            origin = chip(-SIGN[d] * (s + 1))
            return remote(rows(origin, c, h), rows(origin, c, h), ps.at[d, s, h], pr.at[d, s, h], partner)

        def share_in(d, s, h):
            origin = chip(-SIGN[d] * (s + 1))
            return remote(rows(origin, oc, h), rows(origin, oc, h), ps.at[d, s, h], pr.at[d, s, h], partner)

        def own():
            mine = buf.at[pl.ds(pl.multiple_of(j * tb + c * hb, hb), hb)]
            return remote(src, mine, ps.at[0, 3, 1], pr.at[0, 3, 1], partner)

        def keep():
            return pltpu.make_async_copy(src, buf.at[pl.ds(pl.multiple_of(j * tb + c * hb, hb), hb)], keep_sem)

        def start():
            for k in range(2):
                for d in range(2):
                    send(d, 0, FAR[d] if k == 0 else 1 - FAR[d]).start()
            own().start()
            if keep_sem is None:
                buf[pl.ds(pl.multiple_of(j * tb + c * hb, hb), hb), :] = src[...]
            else:
                keep().start()

        units = [(s, k) for s in range(4) for k in range(2) if s < 3 or k == 0]

        def event(e):
            s, k = units[e]
            for d in range(2):
                h = FAR[d] if k == 0 else 1 - FAR[d]
                send(d, s, h).wait_recv()
                if s < 2 or (s == 2 and k == 0):
                    send(d, s + 1, h).start()
                share(d, s, h).start()

        def finish():
            for s, k in units:
                for d in range(2):
                    h = FAR[d] if k == 0 else 1 - FAR[d]
                    share_in(d, s, h).wait_recv()
            own().wait_recv()

        def drain():
            for s, k in units:
                for d in range(2):
                    h = FAR[d] if k == 0 else 1 - FAR[d]
                    send(d, s, h).wait_send()
                    share(d, s, h).wait_send()
            own().wait_send()
            if keep_sem is not None:
                keep().wait()

        return start, event, finish, drain, len(units)

    def scatter_flow(away, own, pbuf, rx, ss, rs, ps, pr, length):
        def share(b, k):
            return remote(away(b, oc), pbuf.at[b], ps.at[k], pr.at[k], partner)

        def part(ref, h):
            return ref.at[pl.ds(h * length, length)]

        def send(d, k, h):
            return remote(part(rx.at[d, k], h), part(rx.at[d, k - 1], h), ss.at[d, k, h], rs.at[d, k - 1, h], core(SIGN[d]))

        def emit(d, k, far, first):
            h = FAR[d] if far else 1 - FAR[d]
            b = chip(SIGN[d] * k)
            if first:
                part(rx.at[d, k], h)[...] = part(own(b), h)[...] + part(pbuf.at[b], h)[...]
            else:
                send(d, k + 1, h).wait_recv()
                part(rx.at[d, k], h)[...] = part(rx.at[d, k], h)[...] + (part(own(b), h)[...] + part(pbuf.at[b], h)[...])
            send(d, k, h).start()

        def final(out):
            for far in (INNER, OUTER):
                for d in range(2):
                    send(d, 1, FAR[d] if far else 1 - FAR[d]).wait_recv()
            out[...] = (own(j)[...] + pbuf[j]) + (rx[0, 0] + rx[1, 0])

        def drain():
            for d in range(2):
                for k, far in ((4, OUTER), (3, INNER), (3, OUTER), (2, INNER), (2, OUTER), (1, INNER), (1, OUTER)):
                    send(d, k, FAR[d] if far else 1 - FAR[d]).wait_send()

        return share, emit, final, drain

    x_start, x_event, x_finish, x_drain, n_units = gather_flow(x_in, xg, x_ss, x_rs, x_ps, x_pr)
    d_start, d_event, d_finish, d_drain, _ = gather_flow(d_in, dg_hbm, d_ss, d_rs, d_ps, d_pr, loc.at[1])
    h_share, h_emit, h_final, h_drain = scatter_flow(
        lambda b, cc: emb_hbm.at[pl.ds(pl.multiple_of(b * tb + cc * hb, hb), hb)], lambda b: ho.at[b], hp, hr, h_ss, h_rs, h_ps, h_pr, half)
    r_share, r_emit, r_final, r_drain = scatter_flow(
        lambda b, cc: dxo.at[b, cc], lambda b: dxo.at[b, c], dxp, dxr, r_ss, r_rs, r_ps, r_pr, dhalf)

    def e_load(b):
        return pltpu.make_async_copy(emb_hbm.at[pl.ds(pl.multiple_of(b * tb + c * hb, hb), hb)], ho.at[b], e_sem.at[b])

    def enter():
        pl.semaphore_wait(barrier, n - 1)
        x_start()
        for k in range(ring):
            h_share(lax.rem(j + k, ring), k).start()

    def h_partner_wait():
        for k in range(ring):
            h_share(lax.rem(j + k, ring), k).wait_recv()
            e_load(k).wait()

    def h_both(k, far, first):
        for d in range(2):
            h_emit(d, k, far, first)

    def h_init():
        h_partner_wait()
        h_both(4, OUTER, FIRST)
        h_both(3, INNER, FIRST)

    side = [
        h_init, d_start,
        lambda: h_both(3, OUTER, LATER), lambda: d_event(0),
        lambda: h_both(2, INNER, LATER), lambda: d_event(1),
        lambda: h_both(2, OUTER, LATER), lambda: d_event(2),
        lambda: h_both(1, INNER, LATER), lambda: d_event(3),
        lambda: h_both(1, OUTER, LATER), lambda: d_event(4),
        lambda: d_event(5), lambda: d_event(6),
    ]

    def at(index, table):
        for when, todo in table:
            def run(when=when, todo=todo):
                with jax.named_scope(f"ev{when}"):
                    todo()

            pl.when(index == when)(run)

    chunk = act_hbm.shape[0] // 4
    n_chunks = act_hbm.shape[0] // chunk
    hid = w1_hbm.shape[1]

    def mlp(w1v, w2v, abuf, ybuf, hbuf, wsem, asem, ysem):
        c1 = pltpu.make_async_copy(w1_hbm, w1v, wsem.at[0])
        c2 = pltpu.make_async_copy(w2_hbm, w2v, wsem.at[1])
        c1.start()

        def a_copy(i):
            slot = lax.rem(i, 2)
            return pltpu.make_async_copy(act_hbm.at[pl.ds(pl.multiple_of(i * chunk, chunk), chunk)], abuf.at[slot], asem.at[slot])

        a_copy(0).start()

        def y_copy(i):
            slot = lax.rem(i, 2)
            return pltpu.make_async_copy(ybuf.at[slot], y_hbm.at[pl.ds(pl.multiple_of(i * chunk, chunk), chunk)], ysem.at[slot])

        c1.wait()
        c2.start()
        w_load.start()
        for b in range(ring):
            e_load(b).start()
        first = [(0, enter), (1, lambda: x_event(1)), (2, lambda: x_event(4)), (3, side[1])]
        second = [(1, lambda: x_event(2)), (2, lambda: x_event(5)), (3, lambda: x_event(6))]
        third = [(0, lambda: x_event(0)), (1, lambda: x_event(3)), (2, side[0]), (3, side[2])]

        @pl.loop(0, n_chunks)
        def _(i):
            slot = lax.rem(i, 2)
            a_copy(i).wait()

            @pl.when(i + 1 < n_chunks)
            def _():
                a_copy(i + 1).start()

            step = min(512, hid // 2)
            per = hid // step

            def up(lo, hi):
                for t in range(lo, hi):
                    u = jnp.dot(abuf[slot], w1v[:, t * step:(t + 1) * step], preferred_element_type=F32)
                    hbuf[:, t * step:(t + 1) * step] = jax.nn.gelu(u).astype(BF16)

            up(0, per // 2)
            at(i, first)
            up(per // 2, per)
            at(i, second)

            @pl.when(i == 0)
            def _():
                c2.wait()

            @pl.when(i >= 2)
            def _():
                y_copy(i - 2).wait()

            for t in range(dim // 256):
                cols = slice(t * 256, (t + 1) * 256)
                low = jnp.dot(hbuf[...], w2v[:, cols], preferred_element_type=F32)
                ybuf[slot, :, cols] = (abuf[slot, :, cols].astype(F32) + low).astype(BF16)
            y_copy(i).start()
            at(i, third)

        y_copy(n_chunks - 2).wait()
        y_copy(n_chunks - 1).wait()

    with jax.named_scope("mlp"):
        pl.run_scoped(
            mlp,
            pltpu.VMEM(w1_hbm.shape, BF16), pltpu.VMEM(w2_hbm.shape, BF16),
            pltpu.VMEM((2, chunk, dim), BF16), pltpu.VMEM((2, chunk, dim), BF16), pltpu.VMEM((chunk, hid), BF16),
            pltpu.SemaphoreType.DMA((2,)), pltpu.SemaphoreType.DMA((2,)), pltpu.SemaphoreType.DMA((2,)),
        )

    def head(z):
        w_load.wait()
        with jax.named_scope("xfinish"):
            x_finish()

        kept = mask_ref[...]
        count = jnp.maximum(jnp.sum(kept, keepdims=True), 1.0)
        wgt[...] = kept / count

        def row_iota(rows):
            return lax.broadcasted_iota(jnp.int32, (rows, tb), 0)

        def logits_phase(zraw):
            @pl.loop(0, ring)
            def _(b):
                xb = xg[pl.ds(pl.multiple_of(b * tb, tb), tb), :]
                lab = lab_ref[pl.ds(b, 1), :]
                tops, sums, tgt = [], [], jnp.zeros((1, tb), F32)
                def logits(q):
                    zt = lax.dot_general(wv[q * QT:(q + 1) * QT, :], xb, NT, preferred_element_type=F32)
                    if (q + 1) * QT > vocab:
                        zt = jnp.where(row_iota(QT) + q * QT < vocab, zt, NEG)
                    zraw[q % 2] = zt

                logits(0)
                for q in range(nq):
                    if q + 1 < nq:
                        logits(q + 1)
                    zt = zraw[q % 2]
                    top = jnp.max(zt, axis=0, keepdims=True)
                    e = jnp.exp(zt - top)
                    z[b, q * QT:(q + 1) * QT, :] = e
                    tgt = tgt + down(jnp.where(row_iota(QT) + q * QT == lab, zt, 0.0))
                    sums.append(down(e))
                    tops.append(top)
                    mst[q, pl.ds(b, 1), :] = top
                peak = functools.reduce(jnp.maximum, tops)
                total = sum(s * jnp.exp(t - peak) for s, t in zip(sums, tops))
                stat_tx[pl.ds(b, 1), :] = peak + jnp.log(total)
                tp_tx[pl.ds(b, 1), :] = tgt * mask_ref[pl.ds(b, 1), :]
                at(b, [(k, side[3 + k]) for k in range(8)])

        with jax.named_scope("logits"):
            pl.run_scoped(logits_phase, pltpu.VMEM((2, QT, tb), F32))

        def stat_copy(p):
            return remote(stat_tx, stat_rx.at[me], st_ss.at[p], st_rs.at[p], {"pp": lax.rem(me + p, n)})

        def tp_copy(p):
            return remote(tp_rx.at[pl.ds(n, 1)], tp_rx.at[pl.ds(me, 1)], tp_ss.at[p], tp_rs.at[p], {"pp": lax.rem(me + p, n)})

        with jax.named_scope("stats"):
            order = [n // 2] + [q for k in range(1, n // 2) for q in (n // 2 - k, n // 2 + k)]
            for p in order:
                stat_copy(p).start()
            stat_rx[me] = stat_tx[...]
            mine = jnp.sum(tp_tx[...], keepdims=True)
            tp_rx[pl.ds(n, 1), :] = jnp.broadcast_to(mine, (1, 128))
            tp_rx[pl.ds(me, 1), :] = jnp.broadcast_to(mine, (1, 128))
            for p in order:
                tp_copy(p).start()

            @pl.loop(0, vpad // 128)
            def _(t):
                o = pl.multiple_of(t * 128, 128)
                wt[:, pl.ds(o, 128)] = wv[pl.ds(o, 128), :].T

            for p in range(1, n):
                stat_copy(p).wait_recv()
            peak = stat_rx[0]
            for p in range(1, n):
                peak = jnp.maximum(peak, stat_rx[p])
            total = jnp.exp(stat_rx[0] - peak)
            for p in range(1, n):
                total = total + jnp.exp(stat_rx[p] - peak)
            lse = peak + jnp.log(total)
            for q in range(nq):
                scale[q] = jnp.exp(mst[q] - lse) * wgt[...]
            lse_sum = jnp.sum(kept * lse, keepdims=True)

        def r_both(k, far, first):
            for d in range(2):
                r_emit(d, k, far, first)

        def dest(t):
            k = jnp.where(t == 0, 4, 3 - (t - 1) // 2)
            k = jnp.where(t == 0, 4, k * (1 - 2 * lax.rem(jnp.maximum(t - 1, 0), 2)))
            return chip(k)

        def pw(t):
            r_share(dest(t), t).wait_recv()

        def first_4():
            pw(0)
            r_both(4, OUTER, FIRST)

        def first_3r():
            pw(1)
            r_emit(0, 3, INNER, FIRST)

        def first_3l():
            pw(2)
            r_emit(1, 3, INNER, FIRST)

        def acc_2():
            pw(3)
            pw(4)
            r_both(2, INNER, LATER)

        dx_events = [(1, first_4), (2, first_3r), (3, first_3l), (5, lambda: r_both(3, OUTER, LATER))]
        dx_side = [(0, side[11]), (1, side[12]), (3, side[13]), (5, lambda: h_final(h0_out))]

        def blocks(gbuf):
            @pl.loop(0, ring)
            def _(t):
                b = dest(t)
                lab = lab_ref[pl.ds(b, 1), :]
                wrow = wgt[pl.ds(b, 1), :]
                for q in range(nq):
                    g = z[b, q * QT:(q + 1) * QT, :] * scale[q, pl.ds(b, 1), :]
                    g = g - jnp.where(row_iota(QT) + q * QT == lab, wrow, 0.0)
                    gbuf[q * QT:(q + 1) * QT, :] = g.astype(BF16)
                res = jnp.dot(wt[...], gbuf[...], preferred_element_type=F32)
                dxo[b, 0] = res[:, :hb]
                dxo[b, 1] = res[:, hb:]
                r_share(b, t).start()
                at(t, dx_events)
                at(t, dx_side)

        with jax.named_scope("dxblocks"):
            pl.run_scoped(blocks, pltpu.VMEM((vpad, tb), BF16))

        def tables(ga, wbuf, wsem):
            def w_copy(i, rows):
                slot = lax.rem(i, 2)
                return pltpu.make_async_copy(wbuf.at[slot, pl.ds(0, rows)], dw_hbm.at[pl.ds(pl.multiple_of(i * WT, 8), rows)], wsem.at[slot])

            tail = vocab - (nw - 1) * WT

            def acc_1():
                pw(5)
                pw(6)
                r_both(1, INNER, LATER)

            dw_events = [(0, acc_2), (3, lambda: r_both(2, OUTER, LATER)), (6, acc_1), (9, lambda: r_both(1, OUTER, LATER))]

            def fill(i, gt):
                o = pl.multiple_of(i * WT, WT)
                q = i // (QT // WT)
                rid = row_iota(WT) + i * WT
                for b in range(ring):
                    g = z[b, pl.ds(o, WT), :] * scale[q, b:b + 1, :]
                    g = g - jnp.where(rid == lab_ref[b:b + 1, :], wgt[b:b + 1, :], 0.0)
                    gt[:, b * tb:(b + 1) * tb] = g.astype(BF16)

            @pl.loop(0, nw)
            def _(i):
                slot = lax.rem(i, 2)
                fill(i, ga)

                @pl.when(i >= 2)
                def _():
                    w_copy(i - 2, WT).wait()

                wbuf[slot] = jnp.dot(ga[...], xg[...], preferred_element_type=F32)

                @pl.when(i < nw - 1)
                def _():
                    w_copy(i, WT).start()

                at(i, dw_events)

            w_copy(nw - 1, tail).start()
            w_copy(nw - 2, WT).wait()
            w_copy(nw - 1, tail).wait()

        d_finish()
        with jax.named_scope("tables"):
            pl.run_scoped(
                tables,
                pltpu.VMEM((WT, ring * tb), BF16),
                pltpu.VMEM((2, WT, dim), F32), pltpu.SemaphoreType.DMA((2,)),
            )

        with jax.named_scope("tail"):
            pw(7)
            r_final(dx_out)
            for p in range(1, n):
                tp_copy(p).wait_recv()
            target = down(tp_rx[0:n, :])
            loss_out[...] = jnp.broadcast_to((lse_sum - target) / count, loss_out.shape)
            for p in range(1, n):
                stat_copy(p).wait_send()
                tp_copy(p).wait_send()
            for t in range(ring):
                r_share(dest(jnp.int32(t)), t).wait_send()

    pl.run_scoped(
        head,
        pltpu.VMEM((ring, vpad, tb), F32),
    )
    with jax.named_scope("drain"):
        x_drain()
        d_drain()
        r_drain()
        h_drain()
        for k in range(ring):
            h_share(lax.rem(j + k, ring), k).wait_send()

def compact(rank, base, cells):
    rows = lax.broadcasted_iota(jnp.int32, (PICK, rank.shape[1]), 0) + base
    for b in range(rank.shape[0]):
        width = rank.shape[1]
        cells[:, b * width:(b + 1) * width] = jnp.where(rows == rank[b:b + 1, :], 1.0, 0.0).astype(BF16)


def positions(cells, digits):
    two = lax.dot_general(digits[...], cells[...], NT, preferred_element_type=F32)
    return (two[0:1] * 64.0 + two[8:9]).astype(jnp.int32)


def pick_rows(vocab, emb_scale, ints, w_hbm, emb, lab, mask, rank, count, digits, wv, cells, hits, sem):
    ring, tb = lab.shape
    vpad = wv.shape[0]
    wv[vpad - 64:, :] = jnp.zeros((64, wv.shape[1]), BF16)
    load = pltpu.make_async_copy(w_hbm, wv.at[pl.ds(0, vocab)], sem)
    load.start()
    offset = lax.axis_index("pp") * vocab
    here = ints[0:ring, :] - offset
    lab[...] = jnp.where((here >= 0) & (here < vocab), here, -1)
    mask[...] = ints[ring:2 * ring, :].astype(F32)
    pos = ints[2 * ring:, :] - offset
    inside = (pos >= 0) & (pos < vocab)
    flag = jnp.where(inside, 1.0, 0.0)
    tri = jnp.where(
        lax.broadcasted_iota(jnp.int32, (tb, tb), 0) <= lax.broadcasted_iota(jnp.int32, (tb, tb), 1), 1.0, 0.0
    ).astype(BF16)
    upto = jnp.dot(flag.astype(BF16), tri, preferred_element_type=F32)
    row = lax.broadcasted_iota(jnp.int32, (ring, tb), 0)
    before = jnp.zeros((1, 1), F32)
    for b in range(ring):
        upto = upto + jnp.where(row == b, before, 0.0)
        before = before + jnp.sum(flag[b:b + 1, :], axis=1, keepdims=True)
    rank[...] = jnp.where(inside, upto.astype(jnp.int32) - 1, -1)
    count[...] = jnp.broadcast_to(before.astype(jnp.int32), count.shape)
    safe = jnp.where(inside, pos, 0)
    for b in range(ring):
        cols = slice(b * tb, (b + 1) * tb)
        digits[0:8, cols] = jnp.broadcast_to((safe[b:b + 1, :] // 64).astype(F32), (8, tb)).astype(BF16)
        digits[8:16, cols] = jnp.broadcast_to(lax.rem(safe[b:b + 1, :], 64).astype(F32), (8, tb)).astype(BF16)
    emb[...] = jnp.zeros(emb.shape, BF16)
    total = jnp.max(before).astype(jnp.int32)
    load.wait()

    @pl.loop(0, (total + PICK - 1) // PICK)
    def _(k):
        compact(rank[...], k * PICK, cells)
        where = positions(cells, digits)
        step = 640
        for v in range(0, vpad, step):
            rows = lax.broadcasted_iota(jnp.int32, (step, PICK), 0) + v
            hits[v:v + step, :] = jnp.where(rows == where, 1.0, 0.0).astype(BF16)
        rows = lax.dot_general(hits[...], wv[...], TN, preferred_element_type=F32)
        rows = (rows * emb_scale).astype(BF16)
        for t in range(0, emb.shape[0], 512):
            spread = lax.dot_general(cells[:, t:t + 512], rows, TN, preferred_element_type=F32)
            emb[t:t + 512, :] = emb[t:t + 512, :] + spread.astype(BF16)


def finish(emb_scale, count, rank, digits, dg, dxt, h0_in, loss_in, acc, y_in, dw, y, dx, h0, loss, cells, picked, where):
    i = pl.program_id(0)
    chunks = (count[0, 0] + PICK - 1) // PICK

    @pl.when(i == 0)
    def _():
        @pl.loop(0, jnp.maximum(chunks, 1))
        def _(k):
            compact(rank[...], k * PICK, cells)
            where[pl.ds(k, 1), :] = positions(cells, digits)
            rows = jnp.dot(cells[...], dg[...], preferred_element_type=F32).astype(BF16)
            picked[pl.ds(pl.multiple_of(k * PICK, PICK), PICK), :] = rows

        dx[...] = dxt[...].T
        h0[...] = h0_in[...]
        loss[...] = loss_in[...]

    y[...] = y_in[...]
    rows = lax.broadcasted_iota(jnp.int32, (acc.shape[0], PICK), 0) + i * acc.shape[0]

    def part(k):
        hits = jnp.where(rows == where[pl.ds(k, 1), :], 1.0, 0.0).astype(BF16)
        return jnp.dot(hits, picked[pl.ds(pl.multiple_of(k * PICK, PICK), PICK), :], preferred_element_type=F32)

    table = lax.fori_loop(1, chunks, lambda k, t: t + part(k), part(0))
    dw[...] = (acc[...] + table * emb_scale).astype(BF16)


def solution(mesh):
    n = mesh.shape["pp"]
    ring = n // 2

    def local_step(x_rows, w_slice, labels, tok_mask, next_ids, d_rows, act_in, w_up, w_down):
        vocab, dim = w_slice.shape
        hb = x_rows.shape[0]
        tb = 2 * hb
        tokens = ring * tb
        vpad = -(-vocab // QT) * QT
        emb_scale = math.sqrt(dim)
        vmem = pl.BlockSpec(memory_space=pltpu.VMEM)
        hbm = pl.BlockSpec(memory_space=pltpu.HBM)
        dma = lambda *s: pltpu.SemaphoreType.DMA(s)
        arr = jax.ShapeDtypeStruct
        ints = jnp.concatenate([labels, tok_mask, next_ids]).reshape(3 * ring, tb)
        emb, lab, mask, rank, count, digits = pl.pallas_call(
            functools.partial(pick_rows, vocab, emb_scale),
            out_shape=[
                arr((tokens, dim), BF16), arr((ring, tb), jnp.int32), arr((ring, tb), F32), arr((ring, tb), jnp.int32),
                arr((8, 128), jnp.int32), arr((16, tokens), BF16),
            ],
            in_specs=[vmem, hbm],
            out_specs=[vmem] * 6,
            scratch_shapes=[
                pltpu.VMEM((vpad, dim), BF16), pltpu.VMEM((PICK, tokens), BF16), pltpu.VMEM((vpad, PICK), BF16), pltpu.SemaphoreType.DMA,
            ],
        )(ints, w_slice)
        dx, acc, h0, y, loss, dg = pl.pallas_call(
            functools.partial(body, n, vocab),
            out_shape=[
                arr((dim, hb), F32), arr((vocab, dim), F32), arr((hb, dim), BF16), arr(act_in.shape[1:], BF16),
                arr((8, 128), F32), arr((tokens, dim), BF16),
            ],
            in_specs=[vmem, vmem, hbm, vmem, vmem, hbm, hbm, hbm, hbm],
            out_specs=[vmem, hbm, vmem, hbm, vmem, hbm],
            scratch_shapes=[
                pltpu.VMEM((vpad, dim), BF16), pltpu.VMEM((dim, vpad), BF16),
                pltpu.VMEM((ring * tb, dim), BF16),
                pltpu.VMEM((ring, 2, dim, hb), F32), pltpu.VMEM((ring, dim, hb), F32), pltpu.VMEM((2, 5, dim, hb), F32),
                pltpu.VMEM((ring, hb, dim), BF16), pltpu.VMEM((ring, hb, dim), BF16), pltpu.VMEM((2, 5, hb, dim), BF16),
                pltpu.VMEM((n, ring, tb), F32), pltpu.VMEM((n + 8, 128), F32),
                pltpu.VMEM((ring, tb), F32), pltpu.VMEM((ring, tb), F32),
                pltpu.VMEM((vpad // QT, ring, tb), F32), pltpu.VMEM((vpad // QT, ring, tb), F32), pltpu.VMEM((ring, tb), F32),
            ] + [dma(2, 4, 2)] * 8 + [dma(2, 5, 2), dma(2, 5, 2), dma(ring), dma(ring)] * 2 + [dma(n)] * 4 + [dma(2), dma(ring)],
            compiler_params=pltpu.CompilerParams(collective_id=0, has_side_effects=True, vmem_limit_bytes=67043328),
        )(x_rows, d_rows, w_slice, lab, mask, act_in[0], w_up[0], w_down[0], emb)
        steps = 8
        vt = -(-vocab // (16 * steps)) * 16
        whole = lambda *s: pl.BlockSpec(s, lambda i: (0, 0))
        tile = lambda rows, cols: pl.BlockSpec((rows, cols), lambda i: (i, 0))
        dw, y, dx, h0, loss = pl.pallas_call(
            functools.partial(finish, emb_scale),
            grid=(steps,),
            out_shape=[
                arr((vocab, dim), BF16), arr(y.shape, BF16), arr((hb, dim), F32), arr((hb, dim), BF16), arr((8, 128), F32),
            ],
            in_specs=[
                pl.BlockSpec(memory_space=pltpu.SMEM), whole(ring, tb), whole(16, tokens), whole(tokens, dim),
                whole(dim, hb), whole(hb, dim), whole(8, 128), tile(vt, dim), tile(y.shape[0] // steps, dim),
            ],
            out_specs=[tile(vt, dim), tile(y.shape[0] // steps, dim), whole(hb, dim), whole(hb, dim), whole(8, 128)],
            scratch_shapes=[
                pltpu.VMEM((PICK, tokens), BF16), pltpu.VMEM((-(-tokens // PICK) * PICK, dim), BF16),
                pltpu.VMEM((max(8, -(-tokens // PICK)), PICK), jnp.int32),
            ],
        )(count, rank, digits, dg, dx, h0, loss, acc, y)
        return loss[0, :1], dx, dw, h0, y[None]

    token_spec = P(("dp", "pp"))
    return jax.shard_map(
        local_step,
        mesh=mesh,
        in_specs=(token_spec, P("pp"), P("dp"), P("dp"), P("dp"), token_spec, token_spec, P("pp"), P("pp")),
        out_specs=(P("dp"), token_spec, token_spec, token_spec, token_spec),
        check_vma=False,
    )
```
